32 devices in a mesh: groups: 1, tok: 32 (over z, y, x, core).
Axes of the slice: x: 2, y: 2, z: 4, core: 2. Of those that a mesh axis runs over, the one named last changes fastest.
Arguments:
- queries: bfloat16 [4096, 2560], P(('groups', 'tok')), may hold values from -5 to 5
- key_rows: bfloat16 [4096, 2560], P(('groups', 'tok')), may hold values from -5 to 5
- value_rows: bfloat16 [4096, 2560], P(('groups', 'tok')), may hold values from -6 to 6
- learn_rates: float32 [4096, 8], P(('groups', 'tok')), may hold values from 0.0002 to 0.002
- frame_order: int32 [4096], P('groups'), may hold values from 0 to 4095, as said below
- window_ids: int32 [4096], P('groups'), may hold values from 0 to 7, never falling along the last dimension, each value on 1 to 2048 neighbouring positions
- fast_init: bfloat16 [640, 3, 2560], replicated, may hold values from -0.3125 to 0.3125
- norm_gain: float32 [2560], replicated, may hold values from 0.5 to 1.5
Outputs:
- layer_out: bfloat16 [4096, 2560], P(('groups', 'tok'))
The draws below stay inside these ranges and needn't reach their ends.
Inputs may be any that keep to these rules, and one draw needn't show every extreme that they name: frame_order[i] is the sequence position of the token stored at row i; every position appears once, and every aligned block of 128 stored rows holds exactly 4 positions of every aligned block of 128 positions.
All inputs are finite; a program needn't handle non-finite values.
Results may differ from the reference program's by a relative error of at most 0.025.
Values may be sent and summed in bfloat16 or wider, within the bound.
A program may use at most 192 MiB of HBM per device.

```python
import math
import jax
import jax.numpy as jnp
import numpy as np
from jax import lax

HEADS = 8
HEAD_DIM = 320
FAST_HID = 640
ATT_DIM = 128
WINDOW = 1024
TOK_DEV = 128
WIDTH = 2560
ATT_HEADS = 20
TOKENS = 4096
SLOTS = 4


def shuffled(sub_key):
    return jax.random.permutation(sub_key, TOK_DEV)


def make_order(key):
    base = jax.random.fold_in(key, 101)
    sources = TOKENS // TOK_DEV
    send_slots = jax.vmap(shuffled)(jax.random.split(jax.random.fold_in(base, 1), sources))
    recv_slots = jax.vmap(shuffled)(jax.random.split(jax.random.fold_in(base, 2), sources))
    source = jnp.arange(sources, dtype=jnp.int32)[:, None]
    target = send_slots // SLOTS
    within = send_slots % SLOTS
    landing = recv_slots[target, source * SLOTS + within]
    return (target * TOK_DEV + landing).reshape(-1).astype(jnp.int32)


def sequence_rows(key, salt):
    noise_key = jax.random.fold_in(key, salt)
    return jnp.clip(jax.random.normal(noise_key, (TOKENS, WIDTH), jnp.float32), -5.0, 5.0)


def draw_frame_order(key, part):
    return make_order(key)


def draw_queries(key, part):
    rows = sequence_rows(key, 202)
    return rows[make_order(key)].astype(jnp.bfloat16)


def draw_key_rows(key, part):
    rows = sequence_rows(key, 404)
    return rows[make_order(key)].astype(jnp.bfloat16)


def steps_of(own_key, dims, cuts, least, largest):
    level, own = 1.0, jax.random.fold_in(own_key, 6)
    for position, blocks in cuts:
        steps = jnp.exp(jax.random.uniform(jax.random.fold_in(own, position), (blocks,), jnp.float32, least / len(cuts), largest / len(cuts)))
        level = level * jnp.repeat(steps, dims[position] // blocks).reshape([-1 if axis == position else 1 for axis in range(len(dims))])
    return level


def split_up(count, total, bound, slope):
    loads = [(1 << 20) // math.isqrt(rank ** slope) + 1 for rank in range(2, count + 1)]
    surplus, given = total - bound - (count - 1), [1] * (count - 1)
    while surplus > 0:
        movable = [i for i in range(count - 1) if given[i] < bound]
        pool, left = sum([loads[i] for i in movable]), surplus
        for i in movable:
            more = min(bound - given[i], max(1, left * loads[i] // pool), surplus)
            given[i] = given[i] + more
            surplus = surplus - more
    return np.array([bound] + given)


def ragged_sizes(stream_key, count, total, most, slope):
    if count == 2:
        one = jax.random.randint(stream_key, (), max(1, total - most), min(most, total - 1) + 1)
        return jnp.stack([one, total - one])
    sizes = jnp.asarray(split_up(count, total, most, slope), jnp.int32)
    twos = (count - 1) // 2
    giver, receiver = sizes[1:1 + 2 * twos:2], sizes[2:2 + 2 * twos:2]
    slack = jnp.minimum(giver - 1, most - receiver)
    passed = jax.random.randint(jax.random.fold_in(stream_key, 1), (twos,), 0, 1 << 20) % (slack + 1)
    sizes = sizes.at[1:1 + 2 * twos:2].set(giver - passed).at[2:2 + 2 * twos:2].set(receiver + passed)
    return sizes[jax.random.permutation(jax.random.fold_in(stream_key, 2), count)]


def normal_values(stream_key, dims, width, bound, pieces=(), kind=jnp.bfloat16):
    values = width * jax.random.normal(stream_key, dims, jnp.float32)
    if pieces:
        values = values * steps_of(stream_key, dims, pieces, -0.22, 0.18)
    return jnp.clip(values, -bound, bound).astype(kind)


def setup_inputs(seed: int = 0, part: int = 0) -> dict:
    splits = jax.random.split(jax.random.key(seed), 9)
    part_keys = jax.random.split(jax.random.fold_in(splits[8], part), 9)
    queries = draw_queries(jax.random.fold_in(jax.random.fold_in(splits[8], part), 71), part)
    key_rows = draw_key_rows(jax.random.fold_in(jax.random.fold_in(splits[8], part), 71), part)
    value_rows = normal_values(part_keys[2], (TOKENS, WIDTH), 1.0, 6.0, ((0, 32),))
    learn_rates = jnp.clip(jnp.exp(math.log(0.002) - 2.3025852 * jax.random.uniform(part_keys[3], (TOKENS, HEADS), jnp.float32) ** steps_of(part_keys[3], (TOKENS, HEADS), ((0, 32),), -0.2, 0.2)), 0.0002, 0.002)
    frame_order = draw_frame_order(jax.random.fold_in(jax.random.fold_in(splits[8], part), 71), part)
    window_ids = jnp.searchsorted(jnp.cumsum(ragged_sizes(part_keys[5], TOKENS // (WINDOW // 2), TOKENS, 2 * WINDOW, 1)), jnp.arange(TOKENS), side="right").astype(jnp.int32)
    fast_init = normal_values(splits[6], (FAST_HID, 3, WIDTH), HEAD_DIM ** -0.5, 0.3125)
    norm_gain = jnp.clip(1.0 + 0.1 * jax.random.normal(splits[7], (WIDTH,), jnp.float32), 0.5, 1.5)
    return {"queries": queries, "key_rows": key_rows, "value_rows": value_rows, "learn_rates": learn_rates, "frame_order": frame_order, "window_ids": window_ids, "fast_init": fast_init, "norm_gain": norm_gain}


epsilon = 1e-06

def rounded(values):
    return lax.optimization_barrier(values.astype(jnp.bfloat16)).astype(jnp.float32)

def head_view(rows):
    return rows.astype(jnp.float32).reshape(rows.shape[0], HEADS, HEAD_DIM)

def matrix_view(weight_rows, which):
    return weight_rows[:, which].astype(jnp.float32).reshape(weight_rows.shape[0], HEADS, HEAD_DIM)

def fast_grads(key_block, value_block, rate_block, weight_rows):
    row_count = weight_rows.shape[0]
    key_heads = head_view(key_block)
    target = rounded(head_view(value_block) * rate_block.astype(jnp.float32)[:, :, None])
    gate = jnp.einsum('thd,jhd->thj', key_heads, matrix_view(weight_rows, 0))
    upward = jnp.einsum('thd,jhd->thj', key_heads, matrix_view(weight_rows, 1))
    backward = jnp.einsum('thd,jhd->thj', target, matrix_view(weight_rows, 2))
    sigmoid = jax.nn.sigmoid(gate)
    active = gate * sigmoid
    product = rounded(active * upward)
    delta_gate = rounded(backward * upward * sigmoid * (1.0 + gate * (1.0 - sigmoid)))
    delta_upper = rounded(backward * active)
    grad_gate = jnp.einsum('thj,thd->jhd', delta_gate, key_heads)
    grad_upper = jnp.einsum('thj,thd->jhd', delta_upper, key_heads)
    grad_down = jnp.einsum('thj,thd->jhd', product, target)
    return jnp.stack([grad_gate.reshape(row_count, WIDTH), grad_upper.reshape(row_count, WIDTH), grad_down.reshape(row_count, WIDTH)], axis=1)

def renormed(base_rows, grads):
    start_rows = base_rows.astype(jnp.float32)
    update = start_rows + grads
    shaped = update.reshape(update.shape[0], 3, HEADS, HEAD_DIM)
    anchor = start_rows.reshape(update.shape[0], 3, HEADS, HEAD_DIM)
    scaling = jnp.sqrt(lax.optimization_barrier(jnp.sum(anchor * anchor, axis=-1, keepdims=True)) + epsilon) / jnp.sqrt(lax.optimization_barrier(jnp.sum(shaped * shaped, axis=-1, keepdims=True)) + epsilon)
    return (shaped * scaling).reshape(update.shape).astype(jnp.bfloat16)

def fast_apply(query_block, weight_rows):
    query_heads = head_view(query_block)
    gate = jnp.einsum('thd,jhd->thj', query_heads, matrix_view(weight_rows, 0))
    upward = jnp.einsum('thd,jhd->thj', query_heads, matrix_view(weight_rows, 1))
    product = rounded(jax.nn.silu(gate) * upward)
    result = jnp.einsum('thj,jhd->thd', product, matrix_view(weight_rows, 2))
    return result.reshape(query_block.shape[0], WIDTH)

def reference(queries, key_rows, value_rows, learn_rates, frame_order, window_ids, fast_init, norm_gain):
    block_count = TOKENS // TOK_DEV
    indices = jnp.arange(block_count, dtype=jnp.int32)

    def accumulate(total, index):
        begin = index * TOK_DEV
        partial_value = fast_grads(lax.dynamic_slice_in_dim(key_rows, begin, TOK_DEV, 0), lax.dynamic_slice_in_dim(value_rows, begin, TOK_DEV, 0), lax.dynamic_slice_in_dim(learn_rates, begin, TOK_DEV, 0), fast_init)
        return (total + rounded(partial_value), jnp.zeros((), jnp.float32))
    grads = lax.scan(accumulate, jnp.zeros((FAST_HID, 3, WIDTH), jnp.float32), indices)[0]
    fresh = renormed(fast_init, grads)
    query_seq = jnp.zeros_like(queries).at[frame_order].set(queries)
    key_seq = jnp.zeros_like(key_rows).at[frame_order].set(key_rows)
    value_seq = jnp.zeros_like(value_rows).at[frame_order].set(value_rows)

    def apply_block(index):
        return fast_apply(lax.dynamic_slice_in_dim(query_seq, index * TOK_DEV, TOK_DEV, 0), fresh)
    fast_out = lax.map(apply_block, indices).reshape(TOKENS, WIDTH)
    half_span = WINDOW // 2
    span = TOK_DEV + 2 * half_span
    key_pad = jnp.pad(key_seq, ((half_span, half_span), (0, 0)))
    value_pad = jnp.pad(value_seq, ((half_span, half_span), (0, 0)))
    ids_pad = jnp.pad(window_ids, (half_span, half_span), constant_values=-1)

    def attend(index):
        begin = index * TOK_DEV
        query_block = lax.dynamic_slice_in_dim(query_seq, begin, TOK_DEV, 0).astype(jnp.float32).reshape(TOK_DEV, ATT_HEADS, ATT_DIM)
        key_block = lax.dynamic_slice_in_dim(key_pad, begin, span, 0).astype(jnp.float32).reshape(span, ATT_HEADS, ATT_DIM)
        value_block = lax.dynamic_slice_in_dim(value_pad, begin, span, 0).astype(jnp.float32).reshape(span, ATT_HEADS, ATT_DIM)
        query_ids = lax.dynamic_slice_in_dim(window_ids, begin, TOK_DEV, 0)
        key_ids = lax.dynamic_slice_in_dim(ids_pad, begin, span, 0)
        query_pos = begin + jnp.arange(TOK_DEV, dtype=jnp.int32)
        key_pos = begin - half_span + jnp.arange(span, dtype=jnp.int32)
        allowed = (key_pos[None, :] >= 0) & (key_pos[None, :] < TOKENS) & (jnp.abs(query_pos[:, None] - key_pos[None, :]) < half_span) & (query_ids[:, None] == key_ids[None, :])
        scores = jnp.einsum('tad,sad->ats', query_block, key_block) * ATT_DIM ** (-0.5)
        scores = jnp.where(allowed[None], scores, -1e+30)
        peak = lax.optimization_barrier(jnp.max(scores, axis=2, keepdims=True))
        weights = jnp.exp(scores - peak)
        total = lax.optimization_barrier(jnp.sum(weights, axis=2, keepdims=True))
        mixed = jnp.einsum('ats,sad->tad', rounded(weights), value_block)
        return (mixed / jnp.transpose(total, (1, 0, 2))).reshape(TOK_DEV, WIDTH)
    attended = lax.map(attend, indices).reshape(TOKENS, WIDTH)
    combined = fast_out + attended
    mean_square = lax.optimization_barrier(jnp.mean(combined * combined, axis=1, keepdims=True))
    return (combined * lax.rsqrt(mean_square + epsilon) * norm_gain).astype(jnp.bfloat16)
```

```python
import functools

import jax
import jax.numpy as jnp
from jax import lax
from jax.experimental import pallas as pl
from jax.experimental.pallas import tpu as pltpu
from jax.sharding import Mesh, PartitionSpec as P

HEADS = 8
ATT_DIM = 128
WINDOW = 1024
SPLIT = 4

epsilon = 1e-06
BF = jnp.bfloat16
F32 = jnp.float32
VM = pl.BlockSpec(memory_space=pltpu.VMEM)
NT = (((1,), (1,)), ((), ()))
TN = (((0,), (0,)), ((), ()))
VMEM_BYTES = 60 * 1024 * 1024


def dot_nt(a, b):
    return lax.dot_general(a, b, NT, preferred_element_type=F32)


def dot_tn(a, b):
    return lax.dot_general(a, b, TN, preferred_element_type=F32)


def dot_nn(a, b):
    return jnp.dot(a, b, preferred_element_type=F32)


def one_hot(left, right):
    return jnp.where(left == right, 1.0, 0.0).astype(BF)


def pack_kernel(span, home, rank_ref, wide_ref, own_ref, query_ref, key_ref, value_ref, out_ref):
    rank = rank_ref[...]
    wide = one_hot(wide_ref[...], rank)
    own = one_hot(own_ref[...], rank)
    groups, width = out_ref.shape[0], out_ref.shape[3]
    keys = dot_nn(wide, key_ref[...]).astype(BF)
    values = dot_nn(wide, value_ref[...]).astype(BF)
    rows = dot_nn(own, query_ref[...]).astype(BF)
    out_ref[:, 0, 0:span, :] = keys.reshape(groups, span, width)
    out_ref[:, 0, span : 2 * span, :] = values.reshape(groups, span, width)
    out_ref[:, 0, 2 * span :, :] = rows.reshape(groups, home, width)


def grads_kernel(span, home, head_dim, recv_ref, rate_ref, weight_ref, out_ref):
    count, _, width = recv_ref.shape
    tokens = count * home
    keys = recv_ref[:, home : 2 * home, :].reshape(tokens, width)
    values = recv_ref[:, span + home : span + 2 * home, :].reshape(tokens, width).astype(F32)
    column = lax.broadcasted_iota(jnp.int32, (1, width), 1)
    for which in range(width // head_dim):
        inside = (column >= which * head_dim) & (column < (which + 1) * head_dim)
        key_part = jnp.where(inside, keys.astype(F32), 0.0).astype(BF)
        target = jnp.where(inside, values * rate_ref[:, which : which + 1], 0.0).astype(BF)
        gate = dot_nt(key_part, weight_ref[0])
        upward = dot_nt(key_part, weight_ref[1])
        backward = dot_nt(target, weight_ref[2])
        sigmoid = jax.nn.sigmoid(gate)
        active = gate * sigmoid
        product = (active * upward).astype(BF)
        delta_gate = (backward * upward * sigmoid * (1.0 + gate * (1.0 - sigmoid))).astype(BF)
        delta_upper = (backward * active).astype(BF)
        parts = (
            dot_tn(delta_gate, key_part),
            dot_tn(delta_upper, key_part),
            dot_tn(product, target),
        )
        for matrix, part in enumerate(parts):
            if which == 0:
                out_ref[matrix] = part.astype(BF)
            else:
                out_ref[matrix] = jnp.where(inside, part, out_ref[matrix].astype(F32)).astype(BF)


def attend_kernel(span, home, chunk, recv_ref, kpos_ref, qpos_ref, low_ref, high_ref, begin_ref, out_ref, query_ref):
    count, _, width = recv_ref.shape
    tokens = count * home
    keys = recv_ref[:, 0:span, :].reshape(count * span, width)
    values = recv_ref[:, span : 2 * span, :].reshape(count * span, width)
    arrived = recv_ref[:, 2 * span :, :].reshape(tokens, width)
    kpos = kpos_ref[...]
    qpos = qpos_ref[...]
    for start in range(0, tokens, chunk):
        place = begin_ref[start : start + chunk, :]
        query = dot_nn(one_hot(place, qpos), arrived).astype(BF)
        query_ref[start : start + chunk, :] = query
        scores = dot_nt(query, keys) * ATT_DIM ** (-0.5)
        allowed = (kpos >= low_ref[start : start + chunk, :]) & (
            kpos < high_ref[start : start + chunk, :]
        )
        scores = jnp.where(allowed, scores, -1e30)
        peak = jnp.max(scores, axis=1, keepdims=True)
        weights = jnp.exp(scores - peak)
        total = jnp.sum(weights, axis=1, keepdims=True)
        out_ref[start : start + chunk, :] = dot_nn(weights.astype(BF), values) / total


def apply_kernel(head_dim, query_ref, weight_ref, grad_ref, attended_ref, out_ref):
    width = query_ref.shape[1]
    column = lax.broadcasted_iota(jnp.int32, (1, width), 1)
    insides = [
        (column >= which * head_dim) & (column < (which + 1) * head_dim)
        for which in range(width // head_dim)
    ]
    fresh = []
    for matrix in range(3):
        base = weight_ref[matrix].astype(F32)
        update = base + grad_ref[matrix].astype(F32)
        base_square = base * base
        update_square = update * update
        scaling = jnp.zeros_like(update)
        for inside in insides:
            old = jnp.sum(jnp.where(inside, base_square, 0.0), axis=1, keepdims=True)
            new = jnp.sum(jnp.where(inside, update_square, 0.0), axis=1, keepdims=True)
            ratio = jnp.sqrt(old + epsilon) / jnp.sqrt(new + epsilon)
            scaling = jnp.where(inside, ratio, scaling)
        fresh.append((update * scaling).astype(BF))
    query = query_ref[...].astype(F32)
    result = attended_ref[...]
    for inside in insides:
        query_part = jnp.where(inside, query, 0.0).astype(BF)
        gate = dot_nt(query_part, fresh[0])
        upward = dot_nt(query_part, fresh[1])
        product = (gate * jax.nn.sigmoid(gate) * upward).astype(BF)
        result = result + jnp.where(inside, dot_nn(product, fresh[2]), 0.0)
    out_ref[...] = result.astype(BF)


def norm_kernel(part_ref, gain_ref, out_ref):
    count, _, width = part_ref.shape
    square = 0.0
    for index in range(count):
        part = part_ref[index].astype(F32)
        square = square + jnp.sum(part * part, axis=1, keepdims=True)
    scale = lax.rsqrt(square / (count * width) + epsilon)
    for index in range(count):
        columns = slice(index * width, (index + 1) * width)
        out_ref[:, columns] = (
            part_ref[index].astype(F32) * scale * gain_ref[:, columns]
        ).astype(BF)


def call(kernel, name, out_shape, flops, size, **options):
    return pl.pallas_call(
        kernel,
        name=name,
        out_shape=out_shape,
        compiler_params=pltpu.CompilerParams(vmem_limit_bytes=VMEM_BYTES),
        cost_estimate=pl.CostEstimate(flops=flops, bytes_accessed=size, transcendentals=0),
        **options,
    )


def shards(
    queries, key_rows, value_rows, learn_rates, frame_order, window_ids, fast_init, norm_gain
):
    tok_dev, model = queries.shape
    groups = lax.axis_size("seg")
    sections = groups * SPLIT
    group = lax.axis_index("seg")
    part = lax.axis_index("hd")
    rank_own = group * SPLIT + part
    slots = tok_dev // sections
    half = WINDOW // 2
    home = SPLIT * slots
    reach = -(-half // tok_dev) * slots
    span = home + 2 * reach
    assert reach == home
    width = model // SPLIT
    head_dim = model // HEADS
    hidden = fast_init.shape[0]
    tokens = sections * home
    counter = jnp.arange(tok_dev, dtype=jnp.int32)

    order = frame_order.reshape(sections, tok_dev)
    sort_key = order // tok_dev * tok_dev + counter[None, :]
    ranks = jnp.sum(
        (sort_key[:, None, :] < sort_key[:, :, None]).astype(jnp.int32), axis=2
    )
    own_rank = lax.dynamic_slice_in_dim(ranks, rank_own, 1, 0)

    wide_want = (
        jnp.arange(groups, dtype=jnp.int32)[:, None] * home
        - reach
        + jnp.arange(span, dtype=jnp.int32)[None, :]
    ).reshape(-1, 1)
    send = call(
        functools.partial(pack_kernel, span, home),
        "pack",
        jax.ShapeDtypeStruct((groups, SPLIT, 2 * span + home, width), BF),
        2 * (2 * groups * span + tok_dev) * tok_dev * model,
        2 * model * (3 * tok_dev + groups * (2 * span + home)),
        grid=(SPLIT,),
        in_specs=[
            pl.BlockSpec((1, tok_dev), lambda h: (0, 0)),
            pl.BlockSpec((groups * span, 1), lambda h: (0, 0)),
            pl.BlockSpec((tok_dev, 1), lambda h: (0, 0)),
            pl.BlockSpec((tok_dev, width), lambda h: (0, h)),
            pl.BlockSpec((tok_dev, width), lambda h: (0, h)),
            pl.BlockSpec((tok_dev, width), lambda h: (0, h)),
        ],
        out_specs=pl.BlockSpec((groups, 1, 2 * span + home, width), lambda h: (0, h, 0, 0)),
    )(own_rank, wide_want, counter[:, None], queries, key_rows, value_rows)
    recv = lax.all_to_all(
        send.reshape(sections, 2 * span + home, width),
        ("seg", "hd"),
        split_axis=0,
        concat_axis=0,
        tiled=True,
    )

    sorting = (own_rank == counter[:, None]).astype(F32)
    rates = jnp.dot(sorting, learn_rates, precision=lax.Precision.HIGHEST)
    rates = rates.reshape(groups, home, SPLIT, HEADS // SPLIT).transpose(0, 2, 1, 3)
    rates = lax.all_to_all(
        rates.reshape(sections, home, HEADS // SPLIT),
        ("seg", "hd"),
        split_axis=0,
        concat_axis=0,
        tiled=True,
    ).reshape(tokens, HEADS // SPLIT)

    wanted = group * home - reach + jnp.arange(span, dtype=jnp.int32)
    match = ranks[:, None, :] == wanted[None, :, None]
    positions = jnp.max(jnp.where(match, order[:, None, :], -1), axis=2)
    kpos = positions.reshape(1, sections * span)
    qpos = positions[:, reach : reach + home].reshape(1, tokens)
    first = group * tokens
    place = first + jnp.arange(tokens, dtype=jnp.int32)
    ids = lax.dynamic_slice_in_dim(window_ids, first, tokens, 0)
    clip_low = jnp.sum((window_ids[None, :] < ids[:, None]).astype(jnp.int32), axis=1)
    clip_high = jnp.sum((window_ids[None, :] <= ids[:, None]).astype(jnp.int32), axis=1)
    low = jnp.maximum(clip_low, place - (half - 1))[:, None]
    high = jnp.minimum(clip_high, place + half)[:, None]

    weight = lax.dynamic_slice_in_dim(fast_init, part * width, width, 2).transpose(1, 0, 2)
    grads = call(
        functools.partial(grads_kernel, span, home, head_dim),
        "grads",
        jax.ShapeDtypeStruct((3, hidden, width), BF),
        24 * tokens * hidden * width,
        4 * tokens * width + 12 * hidden * width,
        in_specs=[VM] * 3,
        out_specs=VM,
    )(recv, rates, weight)
    grads = lax.psum(grads, "seg")

    whole = lambda h: (0, 0)
    attended, query_seq = call(
        functools.partial(attend_kernel, span, home, min(tokens, 128)),
        "attend",
        (
            jax.ShapeDtypeStruct((tokens, width), F32),
            jax.ShapeDtypeStruct((tokens, width), BF),
        ),
        8 * tokens * sections * span * width,
        2 * sections * (2 * span + home) * width + 6 * tokens * width,
        grid=(width // ATT_DIM,),
        in_specs=[
            pl.BlockSpec((sections, 2 * span + home, ATT_DIM), lambda h: (0, 0, h)),
            pl.BlockSpec((1, sections * span), whole),
            pl.BlockSpec((1, tokens), whole),
            pl.BlockSpec((tokens, 1), whole),
            pl.BlockSpec((tokens, 1), whole),
            pl.BlockSpec((tokens, 1), whole),
        ],
        out_specs=(
            pl.BlockSpec((tokens, ATT_DIM), lambda h: (0, h)),
            pl.BlockSpec((tokens, ATT_DIM), lambda h: (0, h)),
        ),
    )(recv, kpos, qpos, low, high, place[:, None])

    combined = call(
        functools.partial(apply_kernel, head_dim),
        "apply",
        jax.ShapeDtypeStruct((tokens, width), BF),
        12 * tokens * hidden * width,
        8 * tokens * width + 12 * hidden * width,
        in_specs=[VM] * 4,
        out_specs=VM,
    )(query_seq, weight, grads, attended)
    returned = lax.all_to_all(
        combined.reshape(SPLIT, tok_dev, width), "hd", split_axis=0, concat_axis=0, tiled=True
    )
    return call(
        norm_kernel,
        "norm",
        jax.ShapeDtypeStruct((tok_dev, model), BF),
        8 * tok_dev * model,
        4 * tok_dev * model,
        in_specs=[VM] * 2,
        out_specs=VM,
    )(returned, norm_gain[None, :])


def solution(mesh):
    count = mesh.shape["tok"]
    split_mesh = Mesh(
        mesh.devices.reshape(mesh.shape["groups"], count // SPLIT, SPLIT),
        ("groups", "seg", "hd"),
    )
    rows = P(("groups", "seg", "hd"), None)
    return jax.shard_map(
        shards,
        mesh=split_mesh,
        in_specs=(rows, rows, rows, rows, P("groups"), P("groups"), P(), P()),
        out_specs=rows,
        check_vma=False,
    )
```
